32 devices in a mesh: dp: 4 (over y, z), tp: 8 (over x, core).
Axes of the slice: x: 4, y: 2, z: 2, core: 2. Of those that a mesh axis runs over, the one named last changes fastest.
The devices are a block of a 4x4x8 slice.
Arguments:
- tokens: bfloat16 [8, 512, 4672], P('dp', 'tp'), parts along dimension 0
- pad_mask: int32 [8, 512], P('dp'), parts along dimension 0
- rel_table: float32 [32, 64], P(None, 'tp')
- w_query: bfloat16 [2, 4672, 4096], P(None, None, 'tp')
- w_key: bfloat16 [2, 4672, 4096], P(None, None, 'tp')
- w_value: bfloat16 [2, 4672, 4096], P(None, None, 'tp')
- w_out: bfloat16 [2, 4096, 4672], P(None, 'tp')
- w_act: bfloat16 [2, 4672, 12352], P(None, None, 'tp')
- w_lin: bfloat16 [2, 4672, 12352], P(None, None, 'tp')
- w_down: bfloat16 [2, 12352, 4672], P(None, 'tp')
- norm_attn: float32 [2, 4672], replicated
- norm_mlp: float32 [2, 4672], replicated
Outputs:
- output: bfloat16 [8, 512, 4672], P('dp', 'tp'), parts along dimension 0
There are 4 independent parts. The reference program is written for one: setup_inputs(seed, part) draws one part's arguments, and reference() takes and returns one part's arrays. A program takes and returns all parts, laid end to end along the dimension named above; an argument that names none is the same for every part.
All inputs are finite; a program needn't handle non-finite values.
Results may differ from the reference program's by a relative error of at most 0.02.
Values are sent between devices in bfloat16 or wider.
A program may use at most 768 MiB of HBM per device.

```python
import jax
import jax.numpy as jnp
from jax import lax

BATCH_SIZE = 2
SEQ_LEN = 512
MODEL_DIM = 4672
NUM_HEADS = 64
HEAD_DIM = 64
FF_DIM = 12352
NUM_LAYERS = 2
NUM_BUCKETS = 32
INNER_DIM = NUM_HEADS * HEAD_DIM


def rel_bucket(offsets):
    side = jnp.where(offsets > 0, 16, 0)
    distance = jnp.minimum(jnp.abs(offsets), 128)
    limits = 64 * 2 ** jnp.arange(1, 8)
    steps = jnp.sum((distance[:, None] * distance[:, None] >= limits[None, :]).astype(jnp.int32), axis=1)
    return side + jnp.where(distance < 8, distance, 8 + steps)


def rms_norm(rows_in, gain_vec):
    rows32 = rows_in.astype(jnp.float32)
    inv_rms = lax.rsqrt(jnp.mean(rows32 * rows32, axis=-1, keepdims=True) + 1e-6)
    return (rows32 * inv_rms * gain_vec).astype(jnp.bfloat16)


def setup_inputs(seed: int = 0, part: int = 0) -> dict:
    root_key = jax.random.key(seed)
    subkeys = jax.random.split(root_key, 10)
    part_keys = jax.random.split(jax.random.fold_in(root_key, part), 3)

    def weight(rng_key, dims, fan_in, factor):
        normal_draw = jax.random.normal(rng_key, dims, jnp.float32)
        return (normal_draw * (factor * fan_in ** -0.5)).astype(jnp.bfloat16)

    tokens = jax.random.normal(part_keys[0], (BATCH_SIZE, SEQ_LEN, MODEL_DIM), jnp.float32).astype(jnp.bfloat16)
    lengths = jax.random.randint(part_keys[1], (BATCH_SIZE,), SEQ_LEN // 8, SEQ_LEN + 1)
    full_row = jax.random.randint(part_keys[2], (), 0, BATCH_SIZE)
    lengths = jnp.where(jnp.arange(BATCH_SIZE) == full_row, SEQ_LEN, lengths)
    pad_mask = (jnp.arange(SEQ_LEN)[None, :] < lengths[:, None]).astype(jnp.int32)
    attn_dims = (NUM_LAYERS, MODEL_DIM, INNER_DIM)
    ff_dims = (NUM_LAYERS, MODEL_DIM, FF_DIM)
    return {
        'tokens': tokens,
        'pad_mask': pad_mask,
        'rel_table': jax.random.normal(subkeys[0], (NUM_BUCKETS, NUM_HEADS), jnp.float32),
        'w_query': weight(subkeys[1], attn_dims, MODEL_DIM * HEAD_DIM, 2.5),
        'w_key': weight(subkeys[2], attn_dims, MODEL_DIM, 1.0),
        'w_value': weight(subkeys[3], attn_dims, MODEL_DIM, 1.0),
        'w_out': weight(subkeys[4], (NUM_LAYERS, INNER_DIM, MODEL_DIM), INNER_DIM, 1.0),
        'w_act': weight(subkeys[5], ff_dims, MODEL_DIM, 1.0),
        'w_lin': weight(subkeys[6], ff_dims, MODEL_DIM, 1.0),
        'w_down': weight(subkeys[7], (NUM_LAYERS, FF_DIM, MODEL_DIM), FF_DIM, 1.0),
        'norm_attn': jax.random.uniform(subkeys[8], (NUM_LAYERS, MODEL_DIM), jnp.float32, 0.5, 1.5),
        'norm_mlp': jax.random.uniform(subkeys[9], (NUM_LAYERS, MODEL_DIM), jnp.float32, 0.5, 1.5),
    }


def reference(tokens, pad_mask, rel_table, w_query, w_key, w_value, w_out, w_act, w_lin, w_down, norm_attn, norm_mlp):
    offsets = jnp.arange(2 * SEQ_LEN - 1) - (SEQ_LEN - 1)
    dist_table = rel_table[rel_bucket(offsets)]
    positions = jnp.arange(SEQ_LEN)
    index = positions[None, :] - positions[:, None] + (SEQ_LEN - 1)
    key_bias = jnp.where(pad_mask == 1, 0.0, -1e9).astype(jnp.float32)
    token_rows = BATCH_SIZE * SEQ_LEN

    def head_attn(operands):
        q_head, k_head, v_head, table_col = operands
        scores = jnp.einsum('bqe,bke->bqk', q_head.astype(jnp.float32), k_head.astype(jnp.float32))
        scores = scores + table_col[index][None] + key_bias[:, None, :]
        attn_probs = jax.nn.softmax(scores, axis=-1).astype(jnp.bfloat16)
        context = jnp.einsum('bqk,bke->bqe', attn_probs.astype(jnp.float32), v_head.astype(jnp.float32))
        return context.astype(jnp.bfloat16)

    def layer(residual, params):
        lay_query, lay_key, lay_value, lay_out, lay_act, lay_lin, lay_down, lay_norm1, lay_norm2 = params
        normed = rms_norm(residual, lay_norm1)

        def project(weight_mat):
            projected = jnp.dot(normed, weight_mat, preferred_element_type=jnp.float32).astype(jnp.bfloat16)
            return projected.reshape(BATCH_SIZE, SEQ_LEN, NUM_HEADS, HEAD_DIM).transpose(2, 0, 1, 3)

        context = lax.map(head_attn, (project(lay_query), project(lay_key), project(lay_value), dist_table.T))
        context = context.transpose(1, 2, 0, 3).reshape(token_rows, INNER_DIM)
        attn_out = jnp.dot(context, lay_out, preferred_element_type=jnp.float32)
        mid_resid = (residual.astype(jnp.float32) + attn_out).astype(jnp.bfloat16)
        normed_mlp = rms_norm(mid_resid, lay_norm2)
        act_proj = jnp.dot(normed_mlp, lay_act, preferred_element_type=jnp.float32)
        lin_proj = jnp.dot(normed_mlp, lay_lin, preferred_element_type=jnp.float32)
        gated = (jax.nn.gelu(act_proj, approximate=True) * lin_proj).astype(jnp.bfloat16)
        ffn_out = jnp.dot(gated, lay_down, preferred_element_type=jnp.float32)
        return (mid_resid.astype(jnp.float32) + ffn_out).astype(jnp.bfloat16), None

    stacked = (w_query, w_key, w_value, w_out, w_act, w_lin, w_down, norm_attn, norm_mlp)
    final_rows, no_out = lax.scan(layer, tokens.reshape(token_rows, MODEL_DIM), stacked)
    return final_rows.reshape(BATCH_SIZE, SEQ_LEN, MODEL_DIM)
```

```python
import functools

import jax
import jax.numpy as jnp
from jax import lax
from jax.experimental import pallas as pl
from jax.experimental.pallas import tpu as pltpu
from jax.sharding import PartitionSpec as P


def rms_norm(rows_in, gain_vec):
    rows32 = rows_in.astype(jnp.float32)
    inv_rms = lax.rsqrt(jnp.mean(rows32 * rows32, axis=-1, keepdims=True) + 1e-6)
    return (rows32 * inv_rms * gain_vec).astype(jnp.bfloat16)


def bias_kernel(seq_len, table_ref, bias_ref):
    head_count = table_ref.shape[0]
    offsets = lax.broadcasted_iota(jnp.int32, (head_count, 2 * seq_len), 1) - seq_len
    distance = jnp.minimum(jnp.abs(offsets), 128)
    bucket = jnp.full_like(distance, 8)
    for step in range(1, 8):
        bucket = bucket + (distance * distance >= 64 * 2 ** step).astype(jnp.int32)
    bucket = jnp.where(distance < 8, distance, bucket) + jnp.where(offsets > 0, 16, 0)
    values = jnp.zeros((head_count, 2 * seq_len), jnp.float32)
    for index in range(table_ref.shape[1]):
        values = jnp.where(bucket == index, table_ref[:, index:index + 1], values)
    for head in range(head_count):
        wide = jnp.broadcast_to(values[head:head + 1], (seq_len, 2 * seq_len))
        bias_ref[head] = pltpu.roll(wide, 0, 1, stride=1, stride_axis=0)[:, seq_len:]


def solution(mesh):
    group_size = mesh.shape['tp']
    col_spec = P(None, None, 'tp')
    row_spec = P(None, 'tp', None)

    def local_fn(tokens, pad_mask, rel_table, w_query, w_key, w_value, w_out, w_act, w_lin, w_down, norm_attn, norm_mlp):
        batch, seq_loc, model_dim = tokens.shape
        seq_len = seq_loc * group_size
        head_count = rel_table.shape[1]
        head_dim = w_query.shape[2] // head_count
        rel_bias = pl.pallas_call(
            functools.partial(bias_kernel, seq_len),
            out_shape=jax.ShapeDtypeStruct((head_count, seq_len, seq_len), jnp.float32),
            name='rel_bias',
        )(rel_table.T)
        key_bias = jnp.where(pad_mask == 1, 0.0, -1e9).astype(jnp.float32)

        def project(gathered, weight_mat):
            projected = jnp.dot(gathered, weight_mat, preferred_element_type=jnp.float32)
            return projected.astype(jnp.bfloat16).reshape(seq_len, head_count, head_dim)

        streams = [tokens[row] for row in range(batch)]
        for layer_idx in range(w_query.shape[0]):
            for row in range(batch):
                residual = streams[row]
                gathered = lax.all_gather(rms_norm(residual, norm_attn[layer_idx]), 'tp', axis=0, tiled=True)
                query_proj = project(gathered, w_query[layer_idx])
                key_proj = project(gathered, w_key[layer_idx])
                value_proj = project(gathered, w_value[layer_idx])
                scores = jnp.einsum('qhe,khe->hqk', query_proj, key_proj, preferred_element_type=jnp.float32)
                attn_probs = jax.nn.softmax(scores + rel_bias + key_bias[row], axis=-1).astype(jnp.bfloat16)
                context = jnp.einsum('hqk,khe->qhe', attn_probs, value_proj, preferred_element_type=jnp.float32).astype(jnp.bfloat16)
                part_out = jnp.dot(context.reshape(seq_len, head_count * head_dim), w_out[layer_idx], preferred_element_type=jnp.float32).astype(jnp.bfloat16)
                attn_out = lax.psum_scatter(part_out, 'tp', scatter_dimension=0, tiled=True)
                streams[row] = (residual.astype(jnp.float32) + attn_out.astype(jnp.float32)).astype(jnp.bfloat16)
            for row in range(batch):
                residual = streams[row]
                gathered = lax.all_gather(rms_norm(residual, norm_mlp[layer_idx]), 'tp', axis=0, tiled=True)
                act_proj = jnp.dot(gathered, w_act[layer_idx], preferred_element_type=jnp.float32)
                lin_proj = jnp.dot(gathered, w_lin[layer_idx], preferred_element_type=jnp.float32)
                gated = (jax.nn.gelu(act_proj, approximate=True) * lin_proj).astype(jnp.bfloat16)
                part_out = jnp.dot(gated, w_down[layer_idx], preferred_element_type=jnp.float32).astype(jnp.bfloat16)
                ffn_out = lax.psum_scatter(part_out, 'tp', scatter_dimension=0, tiled=True)
                streams[row] = (residual.astype(jnp.float32) + ffn_out.astype(jnp.float32)).astype(jnp.bfloat16)
        return jnp.stack(streams)

    in_specs = (P('dp', 'tp', None), P('dp', None), P(None, 'tp'), col_spec, col_spec, col_spec, row_spec,
                col_spec, col_spec, row_spec, P(None, None), P(None, None))
    return jax.shard_map(local_fn, mesh=mesh, in_specs=in_specs, out_specs=P('dp', 'tp', None), check_vma=False)
```

```python
import functools

import jax
import jax.numpy as jnp
from jax import lax
from jax.experimental import pallas as pl
from jax.experimental.pallas import tpu as pltpu
from jax.sharding import PartitionSpec as P

MESH = pl.DeviceIdType.MESH
F32, BF16 = jnp.float32, jnp.bfloat16
TILE = 256
DUE = ((3, 3.5), (4, 8.0), (5, 14.0), (6, 17.5), (7, 21.5), (9, 24.5), (8, 27.5), (10, 31.0))
COST = {'qkv': 1.4, 'attn': 2.5, 'out': 0.75, 'pair': 2.8, 'rest': 1.5, 'down': 2.2}


def plan_steps(pieces):
    table, clock, left = {}, 0.0, list(DUE)
    for name, count in pieces:
        for index in range(count):
            clock += COST[name]
            while left and left[0][1] <= clock:
                table.setdefault((name, index), []).append(left.pop(0)[0])
    table['end'] = [step for step, _ in left]
    return table


def col_tiles(width):
    step = -(-width // (4 * TILE)) * TILE
    return [(start, min(step, width - start)) for start in range(0, width, step)]


def encoder_kernel(group, tokens, key_bias, table, norm_a, norm_m, w_query, w_key, w_value, w_out, w_act, w_lin, w_down,
                   out, h, part, sib, ring, qkv, ctx, gate, toep, wa_buf, wr_buf, wd_buf, wl_buf,
                   rs_send, rs_recv, ag_send, ag_recv, wa_sem, wr_sem, wd_sem, tok_sem):
    layers, dim, inner = w_query.shape
    heads = table.shape[0]
    ff = w_act.shape[2]
    chips = group // 2
    rows = tokens.shape[1]
    seq_len = rows * group
    chunk, half = rows // 2, rows // 4
    n_slot = 4 * layers
    qkv_refs = (w_query, w_key, w_value)
    per_ref = inner // TILE
    n_qkv = 3 * per_ref
    n_pair = ff // TILE
    rest = ff - n_pair * TILE
    tiles = col_tiles(dim)
    q_rows = 128

    me = lax.axis_index('tp')
    x, core = me // 2, me % 2
    right_x, left_x, far_x = (x + 1) % chips, (x + chips - 1) % chips, (x + 2) % chips
    right, left, sibling = right_x * 2 + core, left_x * 2 + core, x * 2 + (1 - core)

    def span(c):
        return pl.ds(c * chunk, chunk)

    def upper(c):
        return pl.ds(c * chunk, half)

    def lower(c):
        return pl.ds(c * chunk + half, half)

    def rs_copy(cs, c, event):
        if event == 6:
            src, dst, dev = part.at[cs, :, 1 - core, span(c)], sib.at[cs, :, span(c)], sibling
        else:
            block = (far_x, right_x, right_x, far_x, left_x, left_x)[event]
            piece = (upper, lower, upper, lower, upper, lower)[event](c)
            src, dst = part.at[cs, block, core, piece], ring.at[cs, event, c]
            dev = right if event < 3 else left
        return pltpu.make_async_remote_copy(src_ref=src, dst_ref=dst, send_sem=rs_send.at[cs, c, event],
                                            recv_sem=rs_recv.at[cs, c, event], device_id={'tp': dev}, device_id_type=MESH)

    def ag_copy(cs, c, event, arriving=False):
        piece = (upper, lower, upper, lower, upper, lower, span, span, span, span)[event](c)
        if arriving:
            block = (left_x, left_x, far_x, right_x, right_x, far_x, x, left_x, right_x, far_x)[event]
            lane = core if event < 6 else 1 - core
        else:
            block = (x, x, left_x, x, x, right_x, x, left_x, right_x, far_x)[event]
            lane = core
        ref = h.at[cs, block, lane, piece]
        dev = right if event < 3 else left if event < 6 else sibling
        return pltpu.make_async_remote_copy(src_ref=ref, dst_ref=ref, send_sem=ag_send.at[cs, c, event],
                                            recv_sem=ag_recv.at[cs, c, event], device_id={'tp': dev}, device_id_type=MESH)

    def arrived(cs, c, event):
        ag_copy(cs, c, event, arriving=True).wait_recv()

    def add_rows(cs, block, piece, other):
        part[cs, block, core, piece] = (part[cs, block, core, piece].astype(F32) + other.astype(F32)).astype(BF16)

    def rs_begin(cs):
        for c in range(2):
            rs_copy(cs, c, 6).start()

    def rs_local(cs, c):
        rs_copy(cs, c, 6).wait_recv()
        add_rows(cs, far_x, span(c), sib[cs, far_x, span(c)])
        rs_copy(cs, c, 0).start()
        rs_copy(cs, c, 3).start()
        add_rows(cs, right_x, span(c), sib[cs, right_x, span(c)])
        rs_copy(cs, c, 1).start()
        add_rows(cs, left_x, span(c), sib[cs, left_x, span(c)])
        rs_copy(cs, c, 4).start()

    def rs_pass(cs, c):
        rs_copy(cs, c, 0).wait_recv()
        add_rows(cs, right_x, upper(c), ring[cs, 0, c])
        rs_copy(cs, c, 2).start()
        rs_copy(cs, c, 3).wait_recv()
        add_rows(cs, left_x, lower(c), ring[cs, 3, c])
        rs_copy(cs, c, 5).start()

    def normalise(cs, c, gain):
        rows32 = out[cs, span(c)].astype(F32)
        inv_rms = lax.rsqrt(jnp.mean(rows32 * rows32, axis=-1, keepdims=True) + 1e-6)
        h[cs, x, core, span(c)] = (rows32 * inv_rms * gain).astype(BF16)

    def ag_begin(cs, c):
        for event in (0, 3, 1, 4, 6):
            ag_copy(cs, c, event).start()

    def gain_of(index):
        row = pl.ds(index // 2, 1)
        return jnp.where(index % 2 == 0, norm_a[row, :], norm_m[row, :])

    def rs_finish(cs, c):
        for event in (1, 2, 4, 5):
            rs_copy(cs, c, event).wait_recv()
        for piece, first, second in ((upper(c), 2, 4), (lower(c), 1, 5)):
            total = part[cs, x, core, piece].astype(F32) + sib[cs, x, piece].astype(F32)
            total = total + ring[cs, first, c].astype(F32) + ring[cs, second, c].astype(F32)
            out[cs, piece] = (out[cs, piece].astype(F32) + total).astype(BF16)

    def ag_forward(cs, c):
        arrived(cs, c, 0)
        ag_copy(cs, c, 2).start()
        arrived(cs, c, 3)
        ag_copy(cs, c, 5).start()

    def ag_share(cs, c):
        arrived(cs, c, 1)
        ag_copy(cs, c, 7).start()
        arrived(cs, c, 4)
        ag_copy(cs, c, 8).start()

    def ag_share_far(cs, c):
        arrived(cs, c, 2)
        arrived(cs, c, 5)
        ag_copy(cs, c, 9).start()

    def ag_end(cs):
        for c in range(2):
            for event in (6, 7, 8, 9):
                arrived(cs, c, event)
        for c in range(2):
            for event in range(10):
                ag_copy(cs, c, event).wait_send()

    def rs_end(cs):
        for c in range(2):
            for event in range(7):
                rs_copy(cs, c, event).wait_send()

    def step(number, slot):
        cs = (slot + 1) % 2
        c = 1 - number % 2 if number < 7 else 0 if number in (7, 9, 11) else 1
        if number in (3, 4):
            @pl.when(slot > 0)
            def _():
                rs_pass(cs, c)
        elif number in (5, 6):
            @pl.when(slot > 0)
            def _():
                rs_finish(cs, c)

                @pl.when(slot < n_slot - 1)
                def _():
                    normalise(cs, c, gain_of((slot + 1) // 2))
                    ag_begin(cs, c)
        else:
            @pl.when(slot < n_slot - 1)
            def _():
                (ag_forward if number in (7, 8) else ag_share if number in (9, 10) else ag_share_far)(cs, c)

    def phase_end(slot, left_over):
        for number in left_over:
            step(number, slot)
        rs_begin(slot % 2)
        rs_local(slot % 2, 0)
        rs_local(slot % 2, 1)
        step(11, slot)
        step(12, slot)

        @pl.when(slot > 0)
        def _():
            rs_end((slot + 1) % 2)

        @pl.when(slot < n_slot - 1)
        def _():
            ag_end((slot + 1) % 2)

    def run_steps(plan, name, index, slot):
        for (piece, at), numbers in [item for item in plan.items() if item[0] != 'end']:
            if piece != name:
                continue
            if isinstance(index, int):
                if index == at:
                    for number in numbers:
                        step(number, slot)
            else:
                @pl.when(index == at)
                def _():
                    for number in numbers:
                        step(number, slot)

    def load_qkv(layer, tile, slot):
        for index, ref in enumerate(qkv_refs):
            @pl.when(tile // per_ref == index)
            def _():
                cols = pl.ds(pl.multiple_of(tile % per_ref * TILE, TILE), TILE)
                pltpu.make_async_copy(ref.at[layer, :, cols], wa_buf.at[slot], wa_sem.at[slot]).start()

    def load_pair(layer, pair, slot):
        cols = pl.ds(pl.multiple_of(pair * TILE, TILE), TILE)
        for index, ref in enumerate((w_act, w_lin)):
            pltpu.make_async_copy(ref.at[layer, :, cols], wa_buf.at[slot + index], wa_sem.at[slot + index]).start()

    def wait_tile(slot):
        pltpu.make_async_copy(w_query.at[0, :, pl.ds(0, TILE)], wa_buf.at[slot], wa_sem.at[slot]).wait()

    def first_qkv(layer):
        for tile in range(min(4, n_qkv)):
            load_qkv(layer, tile, tile)

    def rest_copy(layer, index):
        ref = (w_act, w_lin)[index]
        return pltpu.make_async_copy(ref.at[layer, :, pl.ds(n_pair * TILE, rest)], wr_buf.at[index], wr_sem.at[index])

    def first_pairs(layer):
        for pair in range(min(2, n_pair)):
            load_pair(layer, pair, 2 * pair)
        for index in range(2):
            rest_copy(layer, index).start()

    def down_copy(ref, layer, tile):
        start, width = tiles[tile]
        depth = ref.shape[1]
        last = tile == len(tiles) - 1
        dst = wl_buf.at[pl.ds(0, depth)] if last else wd_buf.at[tile % 2, pl.ds(0, depth)]
        sem = wd_sem.at[2 if last else tile % 2]
        return pltpu.make_async_copy(ref.at[layer, :, pl.ds(start, width)], dst, sem)

    def down_begin(ref, layer):
        down_copy(ref, layer, len(tiles) - 1).start()
        for tile in range(min(2, len(tiles) - 1)):
            down_copy(ref, layer, tile).start()

    def down(ref, layer, seq, slot, left_ref, plan, name):
        depth = ref.shape[1]
        for tile, (start, width) in enumerate(tiles):
            down_copy(ref, layer, tile).wait()
            last = tile == len(tiles) - 1
            weight = wl_buf[pl.ds(0, depth)] if last else wd_buf[tile % 2, pl.ds(0, depth)]
            product = jnp.dot(left_ref[...], weight, preferred_element_type=F32).astype(BF16)
            part[seq, :, :, :, pl.ds(start, width)] = product.reshape(chips, 2, rows, width)
            if tile + 2 < len(tiles) - 1:
                down_copy(ref, layer, tile + 2).start()
            run_steps(plan, name, tile, slot)

    def gathered(seq):
        return h[seq].reshape(seq_len, dim)

    def attention_phase(layer, seq):
        slot = 4 * layer + seq
        plan = plan_steps((('qkv', n_qkv), ('attn', heads // 2), ('out', len(tiles))))
        down_begin(w_out, layer)

        def qkv_tile(tile, carry):
            buf = tile % 4
            wait_tile(buf)
            cols = pl.ds(pl.multiple_of(tile * TILE, TILE), TILE)
            qkv[:, cols] = jnp.dot(gathered(seq), wa_buf[buf], preferred_element_type=F32).astype(BF16)

            @pl.when(tile + 4 < n_qkv)
            def _():
                load_qkv(layer, tile + 4, buf)
            run_steps(plan, 'qkv', tile, slot)
            return carry
        lax.fori_loop(0, n_qkv, qkv_tile, 0)

        @pl.when(seq == 0)
        def _():
            first_qkv(layer)

        @pl.when(seq == 1)
        def _():
            first_pairs(layer)

        def head_pair(pair, carry):
            offset = pl.multiple_of(pair * 128, 128)
            keys = qkv[:, pl.ds(pl.multiple_of(inner + offset, 128), 128)]
            values = qkv[:, pl.ds(pl.multiple_of(2 * inner + offset, 128), 128)]
            mask_row = key_bias[seq]
            for block in range(seq_len // q_rows):
                queries = qkv[pl.ds(block * q_rows, q_rows), pl.ds(offset, 128)]
                lanes = lax.broadcasted_iota(jnp.int32, queries.shape, 1)
                mixed = []
                for side in range(2):
                    mine = jnp.where((lanes < 64) == (side == 0), queries, jnp.zeros_like(queries))
                    scores = lax.dot_general(mine, keys, (((1,), (1,)), ((), ())), preferred_element_type=F32)
                    bias = toep[2 * pair + side, :, pl.ds(seq_len - q_rows - block * q_rows, seq_len)]
                    scores = scores + bias + mask_row
                    weights = jnp.exp(scores - jnp.max(scores, axis=-1, keepdims=True))
                    probs = (weights * (1.0 / jnp.sum(weights, axis=-1, keepdims=True))).astype(BF16)
                    mixed.append(jnp.dot(probs, values, preferred_element_type=F32))
                ctx[pl.ds(block * q_rows, q_rows), pl.ds(offset, 128)] = jnp.where(lanes < 64, mixed[0], mixed[1]).astype(BF16)
            run_steps(plan, 'attn', pair, slot)
            return carry
        lax.fori_loop(0, heads // 2, head_pair, 0)

        down(w_out, layer, seq, slot, ctx, plan, 'out')
        phase_end(slot, plan['end'])

    def mlp_phase(layer, seq):
        slot = 4 * layer + 2 + seq
        plan = plan_steps((('pair', n_pair), ('rest', 1), ('down', len(tiles))))
        down_begin(w_down, layer)

        def pair_tile(pair, carry):
            buf = pair % 2 * 2
            wait_tile(buf)
            act = jnp.dot(gathered(seq), wa_buf[buf], preferred_element_type=F32)
            wait_tile(buf + 1)
            lin = jnp.dot(gathered(seq), wa_buf[buf + 1], preferred_element_type=F32)
            cols = pl.ds(pl.multiple_of(pair * TILE, TILE), TILE)
            gate[:, cols] = (jax.nn.gelu(act, approximate=True) * lin).astype(BF16)

            @pl.when(pair + 2 < n_pair)
            def _():
                load_pair(layer, pair + 2, buf)
            run_steps(plan, 'pair', pair, slot)
            return carry
        lax.fori_loop(0, n_pair, pair_tile, 0)

        for index in range(2):
            rest_copy(layer, index).wait()
        both = jnp.dot(gathered(seq), jnp.concatenate([wr_buf[0], wr_buf[1]], axis=1), preferred_element_type=F32)
        gate[:, n_pair * TILE:] = (jax.nn.gelu(both[:, :rest], approximate=True) * both[:, rest:]).astype(BF16)

        @pl.when(seq == 0)
        def _():
            first_pairs(layer)

        @pl.when((seq == 1) & (layer < layers - 1))
        def _():
            first_qkv(layer + 1)
        run_steps(plan, 'rest', 0, slot)
        down(w_down, layer, seq, slot, gate, plan, 'down')
        phase_end(slot, plan['end'])

    first_qkv(0)
    token_copy = pltpu.make_async_copy(tokens, out, tok_sem)
    token_copy.start()
    barrier = pltpu.get_barrier_semaphore()
    for device in (left, right, sibling):
        pl.semaphore_signal(barrier, inc=1, device_id={'tp': device}, device_id_type=MESH)
    pl.semaphore_wait(barrier, 3)
    token_copy.wait()

    for c in range(2):
        normalise(0, c, norm_a[pl.ds(0, 1), :])
        ag_begin(0, c)
    for c in range(2):
        normalise(1, c, norm_a[pl.ds(0, 1), :])

    offsets = lax.broadcasted_iota(jnp.int32, (heads, 2 * seq_len), 1) - (seq_len - 1)
    distance = jnp.minimum(jnp.abs(offsets), 128)
    bucket = jnp.full_like(distance, 8)
    for power in range(1, 8):
        bucket = bucket + (distance * distance >= 64 * 2 ** power).astype(jnp.int32)
    bucket = jnp.where(distance < 8, distance, bucket) + jnp.where(offsets > 0, 16, 0)
    values = jnp.zeros((heads, 2 * seq_len), F32)
    for index in range(table.shape[1]):
        values = jnp.where(bucket == index, table[:, index:index + 1], values)
    for head in range(heads):
        wide = jnp.broadcast_to(values[head:head + 1], (q_rows, 2 * seq_len))
        toep[head] = pltpu.roll(wide, 2 * seq_len - (q_rows - 1), 1, stride=1, stride_axis=0)[:, :2 * seq_len - q_rows]

    for c in range(2):
        ag_forward(0, c)
    for c in range(2):
        ag_begin(1, c)
    for c in range(2):
        ag_share(0, c)
    for c in range(2):
        ag_share_far(0, c)
    ag_end(0)

    def layer_body(layer, carry):
        for phase in (attention_phase, mlp_phase):
            def one(seq, inner_carry):
                phase(layer, seq)
                return inner_carry
            lax.fori_loop(0, 2, one, 0)
        return carry
    lax.fori_loop(0, layers, layer_body, 0)

    for c in range(2):
        rs_pass(1, c)
    for c in range(2):
        rs_finish(1, c)
    rs_end(1)


def solution(mesh):
    group = mesh.shape['tp']
    col_spec = P(None, None, 'tp')
    row_spec = P(None, 'tp', None)

    def local_fn(tokens, pad_mask, rel_table, w_query, w_key, w_value, w_out, w_act, w_lin, w_down, norm_attn, norm_mlp):
        batch, rows, dim = tokens.shape
        seq_len = rows * group
        heads, inner, ff = rel_table.shape[1], w_query.shape[2], w_act.shape[2]
        rest = ff % TILE
        tiles = col_tiles(dim)
        key_bias = jnp.where(pad_mask == 1, 0.0, -1e9).astype(F32)[:, None, :]
        vmem, hbm = pl.BlockSpec(memory_space=pltpu.VMEM), pl.BlockSpec(memory_space=pl.ANY)
        return pl.pallas_call(
            functools.partial(encoder_kernel, group),
            out_shape=jax.ShapeDtypeStruct(tokens.shape, BF16),
            in_specs=[hbm, vmem, vmem, vmem, vmem] + [hbm] * 7,
            out_specs=vmem,
            scratch_shapes=[
                pltpu.VMEM((batch, group // 2, 2, rows, dim), BF16),
                pltpu.VMEM((batch, group // 2, 2, rows, dim), BF16),
                pltpu.VMEM((2, group // 2, rows, dim), BF16),
                pltpu.VMEM((2, 6, 2, rows // 4, dim), BF16),
                pltpu.VMEM((seq_len, 3 * inner), BF16),
                pltpu.VMEM((seq_len, inner), BF16),
                pltpu.VMEM((seq_len, ff), BF16),
                pltpu.VMEM((heads, 128, 2 * seq_len - 128), F32),
                pltpu.VMEM((4, dim, TILE), BF16),
                pltpu.VMEM((2, dim, rest), BF16),
                pltpu.VMEM((2, ff, tiles[0][1]), BF16),
                pltpu.VMEM((ff, tiles[-1][1]), BF16),
                pltpu.SemaphoreType.DMA((2, 2, 7)),
                pltpu.SemaphoreType.DMA((2, 2, 7)),
                pltpu.SemaphoreType.DMA((2, 2, 10)),
                pltpu.SemaphoreType.DMA((2, 2, 10)),
                pltpu.SemaphoreType.DMA((4,)),
                pltpu.SemaphoreType.DMA((2,)),
                pltpu.SemaphoreType.DMA((3,)),
                pltpu.SemaphoreType.DMA,
            ],
            compiler_params=pltpu.CompilerParams(collective_id=0, has_side_effects=True, vmem_limit_bytes=67_000_000),
            name='encoder',
        )(tokens, key_bias, rel_table.T, norm_attn, norm_mlp, w_query, w_key, w_value, w_out, w_act, w_lin, w_down)

    in_specs = (P('dp', 'tp', None), P('dp', None), P(None, 'tp'), col_spec, col_spec, col_spec, row_spec,
                col_spec, col_spec, row_spec, P(None, None), P(None, None))
    return jax.shard_map(local_fn, mesh=mesh, in_specs=in_specs, out_specs=P('dp', 'tp', None), check_vma=False)
```

```python
import functools

import jax
import jax.numpy as jnp
from jax import lax
from jax.experimental import pallas as pl
from jax.experimental.pallas import tpu as pltpu
from jax.sharding import PartitionSpec as P

MESH = pl.DeviceIdType.MESH
F32, BF16 = jnp.float32, jnp.bfloat16
TILE = 256
N_CHUNK = 2
DUE = {1: (('pass', 0, 8.0), ('finish', 0, 19.0), ('forward', 0, 27.0), ('share', 0, 33.0)),
       2: (('pass', 0, 3.5), ('pass', 1, 8.0), ('finish', 0, 14.0), ('finish', 1, 17.5),
           ('forward', 0, 21.5), ('share', 0, 24.5), ('forward', 1, 27.5), ('share', 1, 31.0))}
COST = {'qkv': 1.9, 'attn': 3.5, 'out': 1.3, 'pair': 2.1, 'rest': 2.2, 'down': 2.1}


def plan_steps(pieces, n_chunk):
    table, clock, left = {}, 0.0, list(DUE[n_chunk])
    for name, count in pieces:
        for index in range(count):
            clock += COST[name]
            while left and left[0][2] <= clock:
                table.setdefault((name, index), []).append(left.pop(0)[:2])
    table['end'] = [item[:2] for item in left]
    return table


def col_tiles(width, pieces):
    step = -(-width // (pieces * TILE)) * TILE
    starts = list(range(0, width, step))
    if len(starts) > 1 and width - starts[-1] <= TILE // 2:
        starts.pop()
    return [(start, end - start) for start, end in zip(starts, starts[1:] + [width])]


def encoder_kernel(group, n_chunk, tokens, pad_mask, table, norm_a, norm_m, w_query, w_key, w_value, w_out, w_act, w_lin, w_down,
                   out, h, part, sib, ring, qkv, ctx, gate, toep, wq_buf, wa_buf, wr_buf, wo_buf, wd_buf, wl_buf,
                   rs_send, rs_recv, ag_send, ag_recv, wq_sem, wa_sem, wr_sem, wo_sem, wd_sem, tok_sem):
    layers, dim, inner = w_query.shape
    heads = table.shape[0]
    ff = w_act.shape[1]
    chips = group // 2
    rows = tokens.shape[1]
    seq_len = rows * group
    chunk, half = rows // n_chunk, rows // n_chunk // 2
    n_slot = 4 * layers
    qkv_refs = (w_query, w_key, w_value)
    per_ref = inner // TILE
    n_qkv = 3 * per_ref
    n_pair = ff // TILE
    rest = ff - n_pair * TILE
    out_tiles, tiles = col_tiles(dim, 4), col_tiles(dim, 6)
    n_wq = wq_buf.shape[0]
    q_rows = 128

    me = lax.axis_index('tp')
    x, core = me // 2, me % 2
    right_x, left_x, far_x = (x + 1) % chips, (x + chips - 1) % chips, (x + 2) % chips
    right, left, sibling = right_x * 2 + core, left_x * 2 + core, x * 2 + (1 - core)

    def span(c):
        return pl.ds(c * chunk, chunk)

    def upper(c):
        return pl.ds(c * chunk, half)

    def lower(c):
        return pl.ds(c * chunk + half, half)

    def rs_copy(cs, c, event):
        if event == 6:
            src, dst, dev = part.at[cs, :, 1 - core, span(c)], sib.at[cs, :, span(c)], sibling
        else:
            block = (far_x, right_x, right_x, far_x, left_x, left_x)[event]
            piece = (upper, lower, upper, lower, upper, lower)[event](c)
            src, dst = part.at[cs, block, core, piece], ring.at[cs, event, c]
            dev = right if event < 3 else left
        return pltpu.make_async_remote_copy(src_ref=src, dst_ref=dst, send_sem=rs_send.at[cs, c, event],
                                            recv_sem=rs_recv.at[cs, c, event], device_id={'tp': dev}, device_id_type=MESH)

    def ag_copy(cs, c, event, arriving=False):
        piece = (upper, lower, upper, lower, upper, lower, span, span, span, span)[event](c)
        if arriving:
            block = (left_x, left_x, far_x, right_x, right_x, far_x, x, left_x, right_x, far_x)[event]
            lane = core if event < 6 else 1 - core
        else:
            block = (x, x, left_x, x, x, right_x, x, left_x, right_x, far_x)[event]
            lane = core
        ref = h.at[cs, block, lane, piece]
        dev = right if event < 3 else left if event < 6 else sibling
        return pltpu.make_async_remote_copy(src_ref=ref, dst_ref=ref, send_sem=ag_send.at[cs, c, event],
                                            recv_sem=ag_recv.at[cs, c, event], device_id={'tp': dev}, device_id_type=MESH)

    def arrived(cs, c, event):
        ag_copy(cs, c, event, arriving=True).wait_recv()

    def add_rows(cs, block, piece, other):
        part[cs, block, core, piece] = (part[cs, block, core, piece].astype(F32) + other.astype(F32)).astype(BF16)

    def rs_begin(cs):
        for c in range(n_chunk):
            rs_copy(cs, c, 6).start()

    def rs_local(cs, c):
        rs_copy(cs, c, 6).wait_recv()
        add_rows(cs, far_x, span(c), sib[cs, far_x, span(c)])
        rs_copy(cs, c, 0).start()
        rs_copy(cs, c, 3).start()
        add_rows(cs, right_x, span(c), sib[cs, right_x, span(c)])
        rs_copy(cs, c, 1).start()
        add_rows(cs, left_x, span(c), sib[cs, left_x, span(c)])
        rs_copy(cs, c, 4).start()

    def rs_pass(cs, c):
        rs_copy(cs, c, 0).wait_recv()
        add_rows(cs, right_x, upper(c), ring[cs, 0, c])
        rs_copy(cs, c, 2).start()
        rs_copy(cs, c, 3).wait_recv()
        add_rows(cs, left_x, lower(c), ring[cs, 3, c])
        rs_copy(cs, c, 5).start()

    def normalise(cs, c, gain):
        rows32 = out[cs, span(c)].astype(F32)
        inv_rms = lax.rsqrt(jnp.mean(rows32 * rows32, axis=-1, keepdims=True) + 1e-6)
        h[cs, x, core, span(c)] = (rows32 * inv_rms * gain).astype(BF16)

    def ag_begin(cs, c):
        for event in (0, 3, 1, 4, 6):
            ag_copy(cs, c, event).start()

    def gain_of(index):
        row = pl.ds(index // 2, 1)
        return jnp.where(index % 2 == 0, norm_a[row, :], norm_m[row, :])

    def rs_finish(cs, c):
        for event in (1, 2, 4, 5):
            rs_copy(cs, c, event).wait_recv()
        for piece, first, second in ((upper(c), 2, 4), (lower(c), 1, 5)):
            total = part[cs, x, core, piece].astype(F32) + sib[cs, x, piece].astype(F32)
            total = total + ring[cs, first, c].astype(F32) + ring[cs, second, c].astype(F32)
            out[cs, piece] = (out[cs, piece].astype(F32) + total).astype(BF16)

    def ag_forward(cs, c):
        arrived(cs, c, 0)
        ag_copy(cs, c, 2).start()
        arrived(cs, c, 3)
        ag_copy(cs, c, 5).start()

    def ag_share(cs, c):
        arrived(cs, c, 1)
        ag_copy(cs, c, 7).start()
        arrived(cs, c, 4)
        ag_copy(cs, c, 8).start()

    def ag_share_far(cs, c):
        arrived(cs, c, 2)
        arrived(cs, c, 5)
        ag_copy(cs, c, 9).start()

    def ag_end(cs):
        for c in range(n_chunk):
            for event in (6, 7, 8, 9):
                arrived(cs, c, event)
        for c in range(n_chunk):
            for event in range(10):
                ag_copy(cs, c, event).wait_send()

    def rs_end(cs):
        for c in range(n_chunk):
            for event in range(7):
                rs_copy(cs, c, event).wait_send()

    def step(item, slot):
        name, c = item
        cs = (slot + 1) % 2
        if name == 'pass':
            @pl.when(slot > 0)
            def _():
                rs_pass(cs, c)
        elif name == 'finish':
            @pl.when(slot > 0)
            def _():
                rs_finish(cs, c)

                @pl.when(slot < n_slot - 1)
                def _():
                    normalise(cs, c, gain_of((slot + 1) // 2))
                    ag_begin(cs, c)
        else:
            @pl.when(slot < n_slot - 1)
            def _():
                {'forward': ag_forward, 'share': ag_share, 'far': ag_share_far}[name](cs, c)

    def phase_end(slot, left_over):
        rs_begin(slot % 2)
        for item in left_over:
            step(item, slot)
        for c in range(n_chunk):
            rs_local(slot % 2, c)
        for c in range(n_chunk):
            step(('far', c), slot)

        @pl.when(slot > 0)
        def _():
            rs_end((slot + 1) % 2)

        @pl.when(slot < n_slot - 1)
        def _():
            ag_end((slot + 1) % 2)

    def run_steps(plan, name, index, slot):
        for (piece, at), items in [entry for entry in plan.items() if entry[0] != 'end']:
            if piece != name:
                continue
            if isinstance(index, int):
                if index == at:
                    for item in items:
                        step(item, slot)
            else:
                @pl.when(index == at)
                def _():
                    for item in items:
                        step(item, slot)

    def load_qkv(layer, tile, slot):
        for index, ref in enumerate(qkv_refs):
            @pl.when(tile // per_ref == index)
            def _():
                cols = pl.ds(pl.multiple_of(tile % per_ref * TILE, TILE), TILE)
                pltpu.make_async_copy(ref.at[layer, :, cols], wq_buf.at[slot], wq_sem.at[slot]).start()

    def load_pair(layer, pair, slot):
        cols = pl.ds(pl.multiple_of(pair * TILE, TILE), TILE)
        for index, ref in enumerate((w_act, w_lin)):
            pltpu.make_async_copy(ref.at[layer, cols, :], wa_buf.at[slot + index], wa_sem.at[slot + index]).start()

    def wait_tile(slot):
        pltpu.make_async_copy(w_act.at[0, pl.ds(0, TILE), :], wa_buf.at[slot], wa_sem.at[slot]).wait()

    def wait_qkv(slot):
        pltpu.make_async_copy(w_query.at[0, :, pl.ds(0, TILE)], wq_buf.at[slot], wq_sem.at[slot]).wait()

    def first_qkv(layer):
        for tile in range(min(n_wq, n_qkv)):
            load_qkv(layer, tile, tile)

    def rest_copy(layer, index):
        ref = (w_act, w_lin)[index]
        return pltpu.make_async_copy(ref.at[layer, pl.ds(n_pair * TILE, rest), :], wr_buf.at[index], wr_sem.at[index])

    def first_pairs(layer):
        for pair in range(min(2, n_pair)):
            load_pair(layer, pair, 2 * pair)
        for index in range(2):
            rest_copy(layer, index).start()

    def out_copy(layer, tile):
        start, width = out_tiles[tile]
        return pltpu.make_async_copy(w_out.at[layer, pl.ds(start, width), :], wo_buf.at[tile % 2, pl.ds(0, width)],
                                     wo_sem.at[tile % 2])

    def down_copy(layer, tile):
        start, width = tiles[tile]
        last = tile == len(tiles) - 1
        dst = wl_buf if last else wd_buf.at[tile % 2]
        return pltpu.make_async_copy(w_down.at[layer, :, pl.ds(start, width)], dst, wd_sem.at[2 if last else tile % 2])

    def keep(seq, start, width, product):
        part[seq, :, :, :, pl.ds(start, width)] = product.astype(BF16).reshape(chips, 2, rows, width)

    def times_rows(left, right):
        return lax.dot_general(left, right, (((1,), (1,)), ((), ())), preferred_element_type=F32)

    def gathered(seq):
        return h[seq].reshape(seq_len, dim)

    def attention_phase(layer, seq):
        slot = 4 * layer + seq
        plan = plan_steps((('qkv', n_qkv), ('attn', heads // 2), ('out', len(out_tiles))), n_chunk)
        for tile in range(min(2, len(out_tiles))):
            out_copy(layer, tile).start()

        def qkv_tile(tile, carry):
            buf = tile % n_wq
            wait_qkv(buf)
            cols = pl.ds(pl.multiple_of(tile * TILE, TILE), TILE)
            qkv[:, cols] = jnp.dot(gathered(seq), wq_buf[buf], preferred_element_type=F32).astype(BF16)

            @pl.when(tile + n_wq < n_qkv)
            def _():
                load_qkv(layer, tile + n_wq, buf)
            run_steps(plan, 'qkv', tile, slot)
            return carry
        lax.fori_loop(0, n_qkv, qkv_tile, 0)

        @pl.when(seq == 0)
        def _():
            first_qkv(layer)

        @pl.when(seq == 1)
        def _():
            first_pairs(layer)

        def head_pair(pair, carry):
            offset = pl.multiple_of(pair * 128, 128)
            keys = qkv[:, pl.ds(pl.multiple_of(inner + offset, 128), 128)]
            values = qkv[:, pl.ds(pl.multiple_of(2 * inner + offset, 128), 128)]
            mask_row = jnp.where(pad_mask[pl.ds(seq, 1), :] == 1, 0.0, -1e9).astype(F32)
            for block in range(seq_len // q_rows):
                queries = qkv[pl.ds(block * q_rows, q_rows), pl.ds(offset, 128)]
                lanes = lax.broadcasted_iota(jnp.int32, queries.shape, 1)
                mixed = []
                for side in range(2):
                    mine = jnp.where((lanes < 64) == (side == 0), queries, jnp.zeros_like(queries))
                    scores = lax.dot_general(mine, keys, (((1,), (1,)), ((), ())), preferred_element_type=F32)
                    bias = toep[2 * pair + side, :, pl.ds(seq_len - q_rows - block * q_rows, seq_len)]
                    scores = scores + bias + mask_row
                    weights = jnp.exp(scores - jnp.max(scores, axis=-1, keepdims=True))
                    probs = (weights * (1.0 / jnp.sum(weights, axis=-1, keepdims=True))).astype(BF16)
                    mixed.append(jnp.dot(probs, values, preferred_element_type=F32))
                ctx[pl.ds(block * q_rows, q_rows), pl.ds(offset, 128)] = jnp.where(lanes < 64, mixed[0], mixed[1]).astype(BF16)
            run_steps(plan, 'attn', pair, slot)
            return carry
        lax.fori_loop(0, heads // 2, head_pair, 0)

        for tile, (start, width) in enumerate(out_tiles):
            out_copy(layer, tile).wait()
            keep(seq, start, width, times_rows(ctx[...], wo_buf[tile % 2, pl.ds(0, width)]))
            if tile + 2 < len(out_tiles):
                out_copy(layer, tile + 2).start()
            run_steps(plan, 'out', tile, slot)
        phase_end(slot, plan['end'])

    def mlp_phase(layer, seq):
        slot = 4 * layer + 2 + seq
        plan = plan_steps((('pair', 2 * n_pair), ('rest', 1), ('down', len(tiles))), n_chunk)
        down_copy(layer, len(tiles) - 1).start()
        for tile in range(min(2, len(tiles) - 1)):
            down_copy(layer, tile).start()

        def pair_tile(pair, carry):
            buf = pair % 2 * 2
            wait_tile(buf)
            act = times_rows(gathered(seq), wa_buf[buf])
            run_steps(plan, 'pair', 2 * pair, slot)
            wait_tile(buf + 1)
            lin = times_rows(gathered(seq), wa_buf[buf + 1])
            cols = pl.ds(pl.multiple_of(pair * TILE, TILE), TILE)
            gate[:, cols] = (jax.nn.gelu(act, approximate=True) * lin).astype(BF16)

            @pl.when(pair + 2 < n_pair)
            def _():
                load_pair(layer, pair + 2, buf)
            run_steps(plan, 'pair', 2 * pair + 1, slot)
            return carry
        lax.fori_loop(0, n_pair, pair_tile, 0)

        for index in range(2):
            rest_copy(layer, index).wait()
        both = times_rows(gathered(seq), jnp.concatenate([wr_buf[0], wr_buf[1]], axis=0))
        gate[:, n_pair * TILE:] = (jax.nn.gelu(both[:, :rest], approximate=True) * both[:, rest:]).astype(BF16)

        @pl.when(seq == 0)
        def _():
            first_pairs(layer)

        @pl.when((seq == 1) & (layer < layers - 1))
        def _():
            first_qkv(layer + 1)
        run_steps(plan, 'rest', 0, slot)
        for tile, (start, width) in enumerate(tiles):
            down_copy(layer, tile).wait()
            weight = wl_buf[...] if tile == len(tiles) - 1 else wd_buf[tile % 2]
            keep(seq, start, width, jnp.dot(gate[...], weight, preferred_element_type=F32))
            if tile + 2 < len(tiles) - 1:
                down_copy(layer, tile + 2).start()
            run_steps(plan, 'down', tile, slot)
        phase_end(slot, plan['end'])

    first_qkv(0)
    token_copy = pltpu.make_async_copy(tokens, out, tok_sem)
    token_copy.start()
    barrier = pltpu.get_barrier_semaphore()
    for device in (left, right, sibling):
        pl.semaphore_signal(barrier, inc=1, device_id={'tp': device}, device_id_type=MESH)
    pl.semaphore_wait(barrier, 3)
    token_copy.wait()

    for c in range(n_chunk):
        normalise(0, c, norm_a[pl.ds(0, 1), :])
        ag_begin(0, c)
    for c in range(n_chunk):
        normalise(1, c, norm_a[pl.ds(0, 1), :])

    offsets = lax.broadcasted_iota(jnp.int32, (heads, 2 * seq_len), 1) - (seq_len - 1)
    distance = jnp.minimum(jnp.abs(offsets), 128)
    bucket = jnp.full_like(distance, 8)
    for power in range(1, 8):
        bucket = bucket + (distance * distance >= 64 * 2 ** power).astype(jnp.int32)
    bucket = jnp.where(distance < 8, distance, bucket) + jnp.where(offsets > 0, 16, 0)
    values = jnp.zeros((heads, 2 * seq_len), F32)
    for index in range(table.shape[1]):
        values = jnp.where(bucket == index, table[:, index:index + 1], values)
    for head in range(heads):
        wide = jnp.broadcast_to(values[head:head + 1], (q_rows, 2 * seq_len))
        toep[head] = pltpu.roll(wide, 2 * seq_len - (q_rows - 1), 1, stride=1, stride_axis=0)[:, :2 * seq_len - q_rows]

    for c in range(n_chunk):
        ag_forward(0, c)
    for c in range(n_chunk):
        ag_begin(1, c)
    for c in range(n_chunk):
        ag_share(0, c)
    for c in range(n_chunk):
        ag_share_far(0, c)
    ag_end(0)

    def layer_body(layer, carry):
        for phase in (attention_phase, mlp_phase):
            def one(seq, inner_carry):
                phase(layer, seq)
                return inner_carry
            lax.fori_loop(0, 2, one, 0)
        return carry
    lax.fori_loop(0, layers, layer_body, 0)

    for c in range(n_chunk):
        rs_pass(1, c)
    for c in range(n_chunk):
        rs_finish(1, c)
    rs_end(1)


def solution(mesh):
    group = mesh.shape['tp']
    col_spec = P(None, None, 'tp')
    row_spec = P(None, 'tp', None)

    def local_fn(tokens, pad_mask, rel_table, w_query, w_key, w_value, w_out, w_act, w_lin, w_down, norm_attn, norm_mlp):
        batch, rows, dim = tokens.shape
        seq_len = rows * group
        heads, inner, ff = rel_table.shape[1], w_query.shape[2], w_act.shape[2]
        rest = ff % TILE
        out_tiles, tiles = col_tiles(dim, 4), col_tiles(dim, 6)
        vmem, hbm = pl.BlockSpec(memory_space=pltpu.VMEM), pl.BlockSpec(memory_space=pl.ANY)
        return pl.pallas_call(
            functools.partial(encoder_kernel, group, N_CHUNK),
            out_shape=jax.ShapeDtypeStruct(tokens.shape, BF16),
            in_specs=[hbm, vmem, vmem, vmem, vmem] + [hbm] * 7,
            out_specs=vmem,
            scratch_shapes=[
                pltpu.VMEM((batch, group // 2, 2, rows, dim), BF16),
                pltpu.VMEM((batch, group // 2, 2, rows, dim), BF16),
                pltpu.VMEM((2, group // 2, rows, dim), BF16),
                pltpu.VMEM((2, 6, N_CHUNK, rows // N_CHUNK // 2, dim), BF16),
                pltpu.VMEM((seq_len, 3 * inner), BF16),
                pltpu.VMEM((seq_len, inner), BF16),
                pltpu.VMEM((seq_len, ff), BF16),
                pltpu.VMEM((heads, 128, 2 * seq_len - 128), F32),
                pltpu.VMEM((2, dim, TILE), BF16),
                pltpu.VMEM((4, TILE, dim), BF16),
                pltpu.VMEM((2, rest, dim), BF16),
                pltpu.VMEM((2, out_tiles[0][1], inner), BF16),
                pltpu.VMEM((2, ff, tiles[0][1]), BF16),
                pltpu.VMEM((ff, tiles[-1][1]), BF16),
                pltpu.SemaphoreType.DMA((2, N_CHUNK, 7)),
                pltpu.SemaphoreType.DMA((2, N_CHUNK, 7)),
                pltpu.SemaphoreType.DMA((2, N_CHUNK, 10)),
                pltpu.SemaphoreType.DMA((2, N_CHUNK, 10)),
                pltpu.SemaphoreType.DMA((2,)),
                pltpu.SemaphoreType.DMA((4,)),
                pltpu.SemaphoreType.DMA((2,)),
                pltpu.SemaphoreType.DMA((2,)),
                pltpu.SemaphoreType.DMA((3,)),
                pltpu.SemaphoreType.DMA,
            ],
            compiler_params=pltpu.CompilerParams(collective_id=0, has_side_effects=True, vmem_limit_bytes=67_000_000),
            name='encoder',
        )(tokens, pad_mask, rel_table.T, norm_attn, norm_mlp, w_query, w_key, w_value, w_out.swapaxes(1, 2),
          w_act.swapaxes(1, 2), w_lin.swapaxes(1, 2), w_down)

    in_specs = (P('dp', 'tp', None), P('dp', None), P(None, 'tp'), col_spec, col_spec, col_spec, row_spec,
                col_spec, col_spec, row_spec, P(None, None), P(None, None))
    return jax.shard_map(local_fn, mesh=mesh, in_specs=in_specs, out_specs=P('dp', 'tp', None), check_vma=False)
```

```python
import functools

import jax
import jax.numpy as jnp
from jax import lax
from jax.experimental import pallas as pl
from jax.experimental.pallas import tpu as pltpu
from jax.sharding import PartitionSpec as P

MESH = pl.DeviceIdType.MESH
F32, BF16 = jnp.float32, jnp.bfloat16
TILE = 256
N_CHUNK = 2
DUE = {1: (('pass', 0, 8.0), ('finish', 0, 19.0), ('forward', 0, 27.0), ('share', 0, 33.0)),
       2: (('pass', 0, 3.5), ('pass', 1, 8.0), ('finish', 0, 14.0), ('finish', 1, 17.5),
           ('forward', 0, 21.5), ('share', 0, 24.5), ('forward', 1, 27.5), ('share', 1, 31.0), ('far', 0, 33.5),
           ('far', 1, 35.5))}
COST = {'qkv': 1.9, 'attn': 3.5, 'out': 1.3, 'pair': 2.1, 'rest': 2.2, 'down': 2.1}


def plan_steps(pieces, n_chunk):
    table, clock, left = {}, 0.0, list(DUE[n_chunk])
    for name, count in pieces:
        for index in range(count):
            clock += COST[name]
            while left and left[0][2] <= clock:
                table.setdefault((name, index), []).append(left.pop(0)[:2])
    table['end'] = [item[:2] for item in left]
    return table


def col_tiles(width, pieces):
    step = -(-width // (pieces * TILE)) * TILE
    starts = list(range(0, width, step))
    if len(starts) > 1 and width - starts[-1] <= TILE // 2:
        starts.pop()
    return [(start, end - start) for start, end in zip(starts, starts[1:] + [width])]


def encoder_kernel(group, n_chunk, tokens, pad_mask, table, norm_a, norm_m, w_query, w_key, w_value, w_out, w_act, w_lin, w_down,
                   out, h, part, sib, ring, qkv, ctx, gate, toep, wq_buf, wa_buf, wr_buf, wo_buf, wd_buf, wl_buf,
                   rs_send, rs_recv, ag_send, ag_recv, wq_sem, wa_sem, wr_sem, wo_sem, wd_sem, tok_sem):
    layers, dim, inner = w_query.shape
    heads = table.shape[0]
    ff = w_act.shape[1]
    chips = group // 2
    rows = tokens.shape[1]
    seq_len = rows * group
    chunk, half = rows // n_chunk, rows // n_chunk // 2
    n_slot = 4 * layers
    qkv_refs = (w_query, w_key, w_value)
    per_ref = inner // TILE
    n_qkv = 3 * per_ref
    n_pair = ff // TILE
    rest = ff - n_pair * TILE
    out_tiles, tiles = col_tiles(dim, 4), col_tiles(dim, 6)
    n_wq = wq_buf.shape[0]
    q_rows = 128

    me = lax.axis_index('tp')
    x, core = me // 2, me % 2
    right_x, left_x, far_x = (x + 1) % chips, (x + chips - 1) % chips, (x + 2) % chips
    right, left, sibling = right_x * 2 + core, left_x * 2 + core, x * 2 + (1 - core)

    def span(c):
        return pl.ds(c * chunk, chunk)

    def upper(c):
        return pl.ds(c * chunk, half)

    def lower(c):
        return pl.ds(c * chunk + half, half)

    def rs_copy(cs, c, event):
        if event == 6:
            src, dst, dev = part.at[cs, :, 1 - core, span(c)], sib.at[cs, :, span(c)], sibling
        else:
            block = (far_x, right_x, right_x, far_x, left_x, left_x)[event]
            piece = (upper, lower, upper, lower, upper, lower)[event](c)
            src, dst = part.at[cs, block, core, piece], ring.at[cs, event, c]
            dev = right if event < 3 else left
        return pltpu.make_async_remote_copy(src_ref=src, dst_ref=dst, send_sem=rs_send.at[cs, c, event],
                                            recv_sem=rs_recv.at[cs, c, event], device_id={'tp': dev}, device_id_type=MESH)

    def ag_copy(cs, c, event, arriving=False):
        piece = (upper, lower, upper, lower, upper, lower, span, span, span, span)[event](c)
        if arriving:
            block = (left_x, left_x, far_x, right_x, right_x, far_x, x, left_x, right_x, far_x)[event]
            lane = core if event < 6 else 1 - core
        else:
            block = (x, x, left_x, x, x, right_x, x, left_x, right_x, far_x)[event]
            lane = core
        ref = h.at[cs, block, lane, piece]
        dev = right if event < 3 else left if event < 6 else sibling
        return pltpu.make_async_remote_copy(src_ref=ref, dst_ref=ref, send_sem=ag_send.at[cs, c, event],
                                            recv_sem=ag_recv.at[cs, c, event], device_id={'tp': dev}, device_id_type=MESH)

    def arrived(cs, c, event):
        ag_copy(cs, c, event, arriving=True).wait_recv()

    def add_rows(cs, block, piece, other):
        part[cs, block, core, piece] = (part[cs, block, core, piece].astype(F32) + other.astype(F32)).astype(BF16)

    def rs_begin(cs):
        for c in range(n_chunk):
            rs_copy(cs, c, 6).start()

    def rs_local(cs, c):
        rs_copy(cs, c, 6).wait_recv()
        add_rows(cs, far_x, span(c), sib[cs, far_x, span(c)])
        rs_copy(cs, c, 0).start()
        rs_copy(cs, c, 3).start()
        add_rows(cs, right_x, span(c), sib[cs, right_x, span(c)])
        rs_copy(cs, c, 1).start()
        add_rows(cs, left_x, span(c), sib[cs, left_x, span(c)])
        rs_copy(cs, c, 4).start()

    def rs_pass(cs, c):
        rs_copy(cs, c, 0).wait_recv()
        add_rows(cs, right_x, upper(c), ring[cs, 0, c])
        rs_copy(cs, c, 2).start()
        rs_copy(cs, c, 3).wait_recv()
        add_rows(cs, left_x, lower(c), ring[cs, 3, c])
        rs_copy(cs, c, 5).start()

    def normalise(cs, c, gain):
        rows32 = out[cs, span(c)].astype(F32)
        inv_rms = lax.rsqrt(jnp.mean(rows32 * rows32, axis=-1, keepdims=True) + 1e-6)
        h[cs, x, core, span(c)] = (rows32 * inv_rms * gain).astype(BF16)

    def ag_begin(cs, c):
        for event in (0, 3, 1, 4, 6):
            ag_copy(cs, c, event).start()

    def gain_of(index):
        row = pl.ds(index // 2, 1)
        return jnp.where(index % 2 == 0, norm_a[row, :], norm_m[row, :])

    def rs_finish(cs, c):
        for event in (1, 2, 4, 5):
            rs_copy(cs, c, event).wait_recv()
        for piece, first, second in ((upper(c), 2, 4), (lower(c), 1, 5)):
            total = part[cs, x, core, piece].astype(F32) + sib[cs, x, piece].astype(F32)
            total = total + ring[cs, first, c].astype(F32) + ring[cs, second, c].astype(F32)
            out[cs, piece] = (out[cs, piece].astype(F32) + total).astype(BF16)

    def ag_forward(cs, c):
        arrived(cs, c, 0)
        ag_copy(cs, c, 2).start()
        arrived(cs, c, 3)
        ag_copy(cs, c, 5).start()

    def ag_share(cs, c):
        arrived(cs, c, 1)
        ag_copy(cs, c, 7).start()
        arrived(cs, c, 4)
        ag_copy(cs, c, 8).start()

    def ag_share_far(cs, c):
        arrived(cs, c, 2)
        arrived(cs, c, 5)
        ag_copy(cs, c, 9).start()

    def ag_end(cs):
        for c in range(n_chunk):
            for event in (6, 7, 8, 9):
                arrived(cs, c, event)
        for c in range(n_chunk):
            for event in range(10):
                ag_copy(cs, c, event).wait_send()

    def rs_end(cs):
        for c in range(n_chunk):
            for event in range(7):
                rs_copy(cs, c, event).wait_send()

    def step(item, slot):
        name, c = item
        cs = (slot + 1) % 2
        if name == 'pass':
            @pl.when(slot > 0)
            def _():
                rs_pass(cs, c)
        elif name == 'finish':
            @pl.when(slot > 0)
            def _():
                rs_finish(cs, c)

                @pl.when(slot < n_slot - 1)
                def _():
                    normalise(cs, c, gain_of((slot + 1) // 2))
                    ag_begin(cs, c)
        else:
            @pl.when(slot < n_slot - 1)
            def _():
                {'forward': ag_forward, 'share': ag_share, 'far': ag_share_far}[name](cs, c)

    def phase_end(slot, left_over):
        rs_begin(slot % 2)
        for item in left_over:
            if item[0] != 'far':
                step(item, slot)
        for c in range(n_chunk):
            rs_local(slot % 2, c)
        for item in left_over:
            if item[0] == 'far':
                step(item, slot)

        @pl.when(slot > 0)
        def _():
            rs_end((slot + 1) % 2)

        @pl.when(slot < n_slot - 1)
        def _():
            ag_end((slot + 1) % 2)

    def run_steps(plan, name, index, slot):
        for (piece, at), items in [entry for entry in plan.items() if entry[0] != 'end']:
            if piece != name:
                continue
            if isinstance(index, int):
                if index == at:
                    for item in items:
                        step(item, slot)
            else:
                @pl.when(index == at)
                def _():
                    for item in items:
                        step(item, slot)

    def load_qkv(layer, tile, slot):
        for index, ref in enumerate(qkv_refs):
            @pl.when(tile // per_ref == index)
            def _():
                cols = pl.ds(pl.multiple_of(tile % per_ref * TILE, TILE), TILE)
                pltpu.make_async_copy(ref.at[layer, :, cols], wq_buf.at[slot], wq_sem.at[slot]).start()

    def load_pair(layer, pair, slot):
        cols = pl.ds(pl.multiple_of(pair * TILE, TILE), TILE)
        for index, ref in enumerate((w_act, w_lin)):
            pltpu.make_async_copy(ref.at[layer, cols, :], wa_buf.at[slot + index], wa_sem.at[slot + index]).start()

    def wait_tile(slot):
        pltpu.make_async_copy(w_act.at[0, pl.ds(0, TILE), :], wa_buf.at[slot], wa_sem.at[slot]).wait()

    def wait_qkv(slot):
        pltpu.make_async_copy(w_query.at[0, :, pl.ds(0, TILE)], wq_buf.at[slot], wq_sem.at[slot]).wait()

    def first_qkv(layer):
        for tile in range(min(n_wq, n_qkv)):
            load_qkv(layer, tile, tile)

    def rest_copy(layer, index):
        ref = (w_act, w_lin)[index]
        return pltpu.make_async_copy(ref.at[layer, pl.ds(n_pair * TILE, rest), :], wr_buf.at[index], wr_sem.at[index])

    def first_pairs(layer):
        for pair in range(min(2, n_pair)):
            load_pair(layer, pair, 2 * pair)
        for index in range(2):
            rest_copy(layer, index).start()

    def out_copy(layer, tile):
        start, width = out_tiles[tile]
        return pltpu.make_async_copy(w_out.at[layer, pl.ds(start, width), :], wo_buf.at[tile % 2, pl.ds(0, width)],
                                     wo_sem.at[tile % 2])

    def down_copy(layer, tile):
        start, width = tiles[tile]
        last = tile == len(tiles) - 1
        dst = wl_buf if last else wd_buf.at[tile % 2]
        return pltpu.make_async_copy(w_down.at[layer, :, pl.ds(start, width)], dst, wd_sem.at[2 if last else tile % 2])

    def keep(seq, start, width, product):
        part[seq, :, :, :, pl.ds(start, width)] = product.astype(BF16).reshape(chips, 2, rows, width)

    def times_rows(left, right):
        return lax.dot_general(left, right, (((1,), (1,)), ((), ())), preferred_element_type=F32)

    def gathered(seq):
        return h[seq].reshape(seq_len, dim)

    def attention_phase(layer, seq):
        slot = 4 * layer + seq
        plan = plan_steps((('qkv', n_qkv), ('attn', heads // 2), ('out', len(out_tiles))), n_chunk)
        for tile in range(min(2, len(out_tiles))):
            out_copy(layer, tile).start()

        def qkv_tile(tile, carry):
            buf = tile % n_wq
            wait_qkv(buf)
            cols = pl.ds(pl.multiple_of(tile * TILE, TILE), TILE)
            qkv[:, cols] = jnp.dot(gathered(seq), wq_buf[buf], preferred_element_type=F32).astype(BF16)

            @pl.when(tile + n_wq < n_qkv)
            def _():
                load_qkv(layer, tile + n_wq, buf)
            run_steps(plan, 'qkv', tile, slot)
            return carry
        lax.fori_loop(0, n_qkv, qkv_tile, 0)

        @pl.when(seq == 0)
        def _():
            first_qkv(layer)

        @pl.when(seq == 1)
        def _():
            first_pairs(layer)

        def head_pair(pair, carry):
            offset = pl.multiple_of(pair * 128, 128)
            keys = qkv[:, pl.ds(pl.multiple_of(inner + offset, 128), 128)]
            values = qkv[:, pl.ds(pl.multiple_of(2 * inner + offset, 128), 128)]
            mask_row = jnp.where(pad_mask[pl.ds(seq, 1), :] == 1, 0.0, -1e9).astype(F32)
            for block in range(seq_len // q_rows):
                queries = qkv[pl.ds(block * q_rows, q_rows), pl.ds(offset, 128)]
                lanes = lax.broadcasted_iota(jnp.int32, queries.shape, 1)
                mixed = []
                for side in range(2):
                    mine = jnp.where((lanes < 64) == (side == 0), queries, jnp.zeros_like(queries))
                    scores = lax.dot_general(mine, keys, (((1,), (1,)), ((), ())), preferred_element_type=F32)
                    bias = toep[2 * pair + side, :, pl.ds(seq_len - q_rows - block * q_rows, seq_len)]
                    scores = scores + bias + mask_row
                    weights = jnp.exp(scores - jnp.max(scores, axis=-1, keepdims=True))
                    probs = (weights * (1.0 / jnp.sum(weights, axis=-1, keepdims=True))).astype(BF16)
                    mixed.append(jnp.dot(probs, values, preferred_element_type=F32))
                ctx[pl.ds(block * q_rows, q_rows), pl.ds(offset, 128)] = jnp.where(lanes < 64, mixed[0], mixed[1]).astype(BF16)
            run_steps(plan, 'attn', pair, slot)
            return carry
        lax.fori_loop(0, heads // 2, head_pair, 0)

        for tile, (start, width) in enumerate(out_tiles):
            out_copy(layer, tile).wait()
            keep(seq, start, width, times_rows(ctx[...], wo_buf[tile % 2, pl.ds(0, width)]))
            if tile + 2 < len(out_tiles):
                out_copy(layer, tile + 2).start()
            run_steps(plan, 'out', tile, slot)
        phase_end(slot, plan['end'])

    def mlp_phase(layer, seq):
        slot = 4 * layer + 2 + seq
        plan = plan_steps((('pair', 2 * n_pair), ('rest', 1), ('down', len(tiles))), n_chunk)
        down_copy(layer, len(tiles) - 1).start()
        for tile in range(min(2, len(tiles) - 1)):
            down_copy(layer, tile).start()

        def pair_tile(pair, carry):
            buf = pair % 2 * 2
            wait_tile(buf)
            act = times_rows(gathered(seq), wa_buf[buf])
            run_steps(plan, 'pair', 2 * pair, slot)
            wait_tile(buf + 1)
            lin = times_rows(gathered(seq), wa_buf[buf + 1])
            cols = pl.ds(pl.multiple_of(pair * TILE, TILE), TILE)
            gate[:, cols] = (jax.nn.gelu(act, approximate=True) * lin).astype(BF16)

            @pl.when(pair + 2 < n_pair)
            def _():
                load_pair(layer, pair + 2, buf)
            run_steps(plan, 'pair', 2 * pair + 1, slot)
            return carry
        lax.fori_loop(0, n_pair, pair_tile, 0)

        for index in range(2):
            rest_copy(layer, index).wait()
        both = times_rows(gathered(seq), jnp.concatenate([wr_buf[0], wr_buf[1]], axis=0))
        gate[:, n_pair * TILE:] = (jax.nn.gelu(both[:, :rest], approximate=True) * both[:, rest:]).astype(BF16)

        @pl.when(seq == 0)
        def _():
            first_pairs(layer)

        @pl.when((seq == 1) & (layer < layers - 1))
        def _():
            first_qkv(layer + 1)
        run_steps(plan, 'rest', 0, slot)
        for tile, (start, width) in enumerate(tiles):
            down_copy(layer, tile).wait()
            weight = wl_buf[...] if tile == len(tiles) - 1 else wd_buf[tile % 2]
            keep(seq, start, width, jnp.dot(gate[...], weight, preferred_element_type=F32))
            if tile + 2 < len(tiles) - 1:
                down_copy(layer, tile + 2).start()
            run_steps(plan, 'down', tile, slot)
        phase_end(slot, plan['end'])

    first_qkv(0)
    token_copy = pltpu.make_async_copy(tokens, out, tok_sem)
    token_copy.start()
    barrier = pltpu.get_barrier_semaphore()
    for device in (left, right, sibling):
        pl.semaphore_signal(barrier, inc=1, device_id={'tp': device}, device_id_type=MESH)
    pl.semaphore_wait(barrier, 3)
    token_copy.wait()

    for c in range(n_chunk):
        normalise(0, c, norm_a[pl.ds(0, 1), :])
        ag_begin(0, c)
    for c in range(n_chunk):
        normalise(1, c, norm_a[pl.ds(0, 1), :])

    offsets = lax.broadcasted_iota(jnp.int32, (heads, 2 * seq_len), 1) - (seq_len - 1)
    distance = jnp.minimum(jnp.abs(offsets), 128)
    bucket = jnp.full_like(distance, 8)
    for power in range(1, 8):
        bucket = bucket + (distance * distance >= 64 * 2 ** power).astype(jnp.int32)
    bucket = jnp.where(distance < 8, distance, bucket) + jnp.where(offsets > 0, 16, 0)
    values = jnp.zeros((heads, 2 * seq_len), F32)
    for index in range(table.shape[1]):
        values = jnp.where(bucket == index, table[:, index:index + 1], values)
    for head in range(heads):
        wide = jnp.broadcast_to(values[head:head + 1], (q_rows, 2 * seq_len))
        toep[head] = pltpu.roll(wide, 2 * seq_len - (q_rows - 1), 1, stride=1, stride_axis=0)[:, :2 * seq_len - q_rows]

    for c in range(n_chunk):
        ag_forward(0, c)
    for c in range(n_chunk):
        ag_begin(1, c)
    for c in range(n_chunk):
        ag_share(0, c)
    for c in range(n_chunk):
        ag_share_far(0, c)
    ag_end(0)

    def layer_body(layer, carry):
        for phase in (attention_phase, mlp_phase):
            def one(seq, inner_carry):
                phase(layer, seq)
                return inner_carry
            lax.fori_loop(0, 2, one, 0)
        return carry
    lax.fori_loop(0, layers, layer_body, 0)

    for c in range(n_chunk):
        rs_pass(1, c)
    for c in range(n_chunk):
        rs_finish(1, c)
    rs_end(1)


def solution(mesh):
    group = mesh.shape['tp']
    col_spec = P(None, None, 'tp')
    row_spec = P(None, 'tp', None)

    def local_fn(tokens, pad_mask, rel_table, w_query, w_key, w_value, w_out, w_act, w_lin, w_down, norm_attn, norm_mlp):
        batch, rows, dim = tokens.shape
        seq_len = rows * group
        heads, inner, ff = rel_table.shape[1], w_query.shape[2], w_act.shape[2]
        rest = ff % TILE
        out_tiles, tiles = col_tiles(dim, 4), col_tiles(dim, 6)
        vmem, hbm = pl.BlockSpec(memory_space=pltpu.VMEM), pl.BlockSpec(memory_space=pl.ANY)
        return pl.pallas_call(
            functools.partial(encoder_kernel, group, N_CHUNK),
            out_shape=jax.ShapeDtypeStruct(tokens.shape, BF16),
            in_specs=[hbm, vmem, vmem, vmem, vmem] + [hbm] * 7,
            out_specs=vmem,
            scratch_shapes=[
                pltpu.VMEM((batch, group // 2, 2, rows, dim), BF16),
                pltpu.VMEM((batch, group // 2, 2, rows, dim), BF16),
                pltpu.VMEM((2, group // 2, rows, dim), BF16),
                pltpu.VMEM((2, 6, N_CHUNK, rows // N_CHUNK // 2, dim), BF16),
                pltpu.VMEM((seq_len, 3 * inner), BF16),
                pltpu.VMEM((seq_len, inner), BF16),
                pltpu.VMEM((seq_len, ff), BF16),
                pltpu.VMEM((heads, 128, 2 * seq_len - 128), F32),
                pltpu.VMEM((2, dim, TILE), BF16),
                pltpu.VMEM((4, TILE, dim), BF16),
                pltpu.VMEM((2, rest, dim), BF16),
                pltpu.VMEM((2, out_tiles[0][1], inner), BF16),
                pltpu.VMEM((2, ff, tiles[0][1]), BF16),
                pltpu.VMEM((ff, tiles[-1][1]), BF16),
                pltpu.SemaphoreType.DMA((2, N_CHUNK, 7)),
                pltpu.SemaphoreType.DMA((2, N_CHUNK, 7)),
                pltpu.SemaphoreType.DMA((2, N_CHUNK, 10)),
                pltpu.SemaphoreType.DMA((2, N_CHUNK, 10)),
                pltpu.SemaphoreType.DMA((2,)),
                pltpu.SemaphoreType.DMA((4,)),
                pltpu.SemaphoreType.DMA((2,)),
                pltpu.SemaphoreType.DMA((2,)),
                pltpu.SemaphoreType.DMA((3,)),
                pltpu.SemaphoreType.DMA,
            ],
            compiler_params=pltpu.CompilerParams(collective_id=0, has_side_effects=True, vmem_limit_bytes=67_000_000),
            name='encoder',
        )(tokens, pad_mask, rel_table.T, norm_attn, norm_mlp, w_query, w_key, w_value, w_out.swapaxes(1, 2),
          w_act.swapaxes(1, 2), w_lin.swapaxes(1, 2), w_down)

    in_specs = (P('dp', 'tp', None), P('dp', None), P(None, 'tp'), col_spec, col_spec, col_spec, row_spec,
                col_spec, col_spec, row_spec, P(None, None), P(None, None))
    return jax.shard_map(local_fn, mesh=mesh, in_specs=in_specs, out_specs=P('dp', 'tp', None), check_vma=False)
```
